32 devices in a mesh: src: 4 (over z), tile: 8 (over y, x, core).
Axes of the slice: x: 2, y: 2, z: 4, core: 2. Of those that a mesh axis runs over, the one named last changes fastest.
Arguments:
- tables: float32 [32, 32, 32, 1024], P(('src', 'tile')), may hold values from 0.2 to 2
- weights: float32 [32, 32], P(('src', 'tile')), may hold values from 0.05 to 0.5
- aperture: int32 [32, 32], P(('src', 'tile')), may hold values from 0 to 1, as said below
Outputs:
- image: float32 [32, 64, 32, 128], P('tile', 'src')
The draws below stay inside these ranges and needn't reach their ends.
Inputs may be any that keep to these rules, and one draw needn't show every extreme that they name: `aperture`: within one source and one group of 4 consecutive tiles (g * 4 to g * 4 + 3), at most 2 entries are 1; some group has exactly 2 for every source.
All inputs are finite; a program needn't handle non-finite values.
Results may differ from the reference program's by a relative error of at most 0.0003.
Values sent between devices are 32-bit elements; how exact they have to be, the bound alone decides.
No kernel may reach another device: no remote copies, remote signals or barrier semaphores. Data moves between devices by JAX's collectives and lax.ppermute only.
A program may use at most 128 MiB of HBM per device.

```python
import math
import jax
import jax.numpy as jnp
from jax import lax

BX = 32
BY = 16
BZ = 64
BRICKS = 32
SOURCES = 32
GROUP = 4
CAP = 2


def draw_aperture(key, part):
    keys = jax.random.split(jax.random.fold_in(key, 17), 5)
    groups = BRICKS // GROUP
    heated = jax.random.randint(keys[0], (groups,), 0, 4) == 0
    filled_group = jax.random.randint(keys[1], (), 0, groups)
    group_ids = jnp.arange(groups)
    chance = jnp.where(heated, 85, 15)
    rolled = jax.random.randint(keys[2], (SOURCES, groups), 0, 100)
    partial_count = jax.random.randint(keys[3], (SOURCES, groups), 0, CAP)
    counts = jnp.where(rolled < chance[None, :], CAP, partial_count)
    counts = jnp.where(group_ids[None, :] == filled_group, CAP, counts)
    scores = jax.random.randint(keys[4], (SOURCES, groups, GROUP), 0, 1 << 20) * GROUP + jnp.arange(GROUP)
    ranking = jnp.sum((scores[:, :, None, :] < scores[:, :, :, None]).astype(jnp.int32), axis=3)
    chosen = ranking < counts[:, :, None]
    return chosen.reshape(SOURCES, BRICKS).astype(jnp.int32)


def level_of(rng, extent, cuts, smallest, largest):
    def one(dim, parts):
        draws = jax.random.uniform(jax.random.fold_in(jax.random.fold_in(rng, 6), dim), (parts,), jnp.float32, smallest / len(cuts), largest / len(cuts))
        return jnp.repeat(jnp.exp(draws), extent[dim] // parts).reshape((-1,) + (1,) * (len(extent) - dim - 1))

    gain = one(*cuts[0])
    for cut in cuts[1:]:
        gain = gain * one(*cut)
    return gain


def setup_inputs(seed: int = 0) -> dict:
    arg_keys = jax.random.split(jax.random.key(seed), 4)
    tables = jnp.clip(0.2 + 1.8 * jax.random.uniform(arg_keys[0], (SOURCES, BRICKS, BX, BY * BZ), jnp.float32) ** level_of(arg_keys[0], (SOURCES, BRICKS, BX, BY * BZ), ((0, 32),), -0.2, 0.2), 0.2, 2.0)
    weights = jnp.clip(jnp.exp(math.log(0.5) - 2.3025851 * jax.random.uniform(arg_keys[1], (SOURCES, BRICKS), jnp.float32) ** level_of(arg_keys[1], (SOURCES, BRICKS), ((0, 32),), -0.2, 0.2)), 0.05, 0.5)
    aperture = draw_aperture(jax.random.fold_in(arg_keys[3], 71), 0)
    return {"tables": tables, "weights": weights, "aperture": aperture}


angular_rate = 9.0


def refine_matrix(length):
    rows = jnp.arange(2 * length)
    cols = jnp.arange(length)
    center = rows // 2
    other = jnp.where(rows % 2 == 0, jnp.maximum(center - 1, 0), jnp.minimum(center + 1, length - 1))
    near = (cols[None, :] == center[:, None]).astype(jnp.float32)
    away = (cols[None, :] == other[:, None]).astype(jnp.float32)
    return 0.75 * near + 0.25 * away


def refine_all(bricks, rows_matrix, y_matrix, z_matrix):
    count = bricks.shape[0]
    fine_rows = rows_matrix.shape[0]
    along_x = jnp.einsum('fr,krc->kfc', rows_matrix, bricks, precision=lax.Precision.HIGHEST)
    flat = along_x.reshape(count * fine_rows * BY, BZ)
    along_z = jnp.dot(flat, z_matrix.T, precision=lax.Precision.HIGHEST).reshape(count, fine_rows, BY, 2 * BZ)
    return jnp.einsum('Yy,kfyz->kfYz', y_matrix, along_z, precision=lax.Precision.HIGHEST)


def reference(tables, weights, aperture):
    x_matrix = refine_matrix(BX)
    y_matrix = refine_matrix(BY)
    z_matrix = refine_matrix(BZ)
    scale = weights * aperture.astype(jnp.float32)

    def one_source(total, item):
        bricks, factor = item
        fine = refine_all(bricks, x_matrix, y_matrix, z_matrix)
        return total + factor[:, None, None, None] * jnp.cos(angular_rate * fine), None

    start = jnp.zeros((BRICKS, 2 * BX, 2 * BY, 2 * BZ), jnp.float32)
    total, unused = lax.scan(one_source, start, (tables, scale))
    return total
```

```python
import functools
import math

import jax
import jax.numpy as jnp
import numpy as np
from jax import lax
from jax.experimental import pallas as pl
from jax.experimental.pallas import tpu as pltpu
from jax.sharding import PartitionSpec as P

BX = 32
BY = 16
BZ = 64
SUB = 8
LANES = 128

angular_rate = 9.0


def refine_axis(values, axis):
    length = values.shape[axis]
    first = lax.slice_in_dim(values, 0, 1, axis=axis)
    last = lax.slice_in_dim(values, length - 1, length, axis=axis)
    lower = jnp.concatenate([first, lax.slice_in_dim(values, 0, length - 1, axis=axis)], axis=axis)
    upper = jnp.concatenate([lax.slice_in_dim(values, 1, length, axis=axis), last], axis=axis)
    even_rows = 0.75 * values + 0.25 * lower
    odd_rows = 0.75 * values + 0.25 * upper
    paired = jnp.stack([even_rows, odd_rows], axis=axis + 1)
    shape = values.shape[:axis] + (2 * length,) + values.shape[axis + 1 :]
    return paired.reshape(shape)


def refine_accumulate(coarse, details, fine_rows, tile_count):
    items = coarse.shape[0]
    turns = 8
    block = items // turns
    coarse_rows = coarse.shape[1]
    tile_ids = jnp.arange(tile_count).astype(jnp.float32)

    def one_block(total, item):
        bricks, info = item
        shaped = bricks.reshape(block, coarse_rows, BY, BZ)
        along_x = refine_axis(shaped, 1)
        along_z = refine_axis(along_x, 3)
        fine = refine_axis(along_z, 2)
        phase = jnp.cos(angular_rate * fine)
        select = (info[:, 1:2] == tile_ids[None, :]).astype(jnp.float32) * info[:, 0:1]
        total = total + jnp.einsum("kp,kfyz->pfyz", select, phase, precision=lax.Precision.HIGHEST)
        return (total, None)

    stacked = (
        coarse.reshape(turns, block, coarse_rows, coarse.shape[2]),
        details.reshape(turns, block, 2),
    )
    start = jnp.zeros((tile_count, fine_rows, 2 * BY, 2 * BZ), jnp.float32)
    total, unused = lax.scan(one_block, start, stacked)
    return total


def general_shards(tables, weights, aperture):
    bricks = tables[0]
    own_weight = weights[0]
    own_mask = aperture[0]
    owners = lax.axis_size("tile")
    group = bricks.shape[0] // owners
    capacity = group // 2
    plane = bricks.shape[2]
    live = own_mask.reshape(owners, group)
    ranking = jnp.cumsum(live, axis=1) - 1
    slot_ids = jnp.arange(capacity)
    chosen = ((live[:, None, :] == 1) & (ranking[:, None, :] == slot_ids[None, :, None])).astype(
        jnp.int32
    )
    local_tile = jnp.sum(chosen * jnp.arange(group)[None, None, :], axis=2)
    occupied = jnp.sum(chosen, axis=2)
    brick_index = local_tile + jnp.arange(owners)[:, None] * group
    picked = bricks[brick_index]
    factor = own_weight[brick_index] * occupied.astype(jnp.float32)
    details = jnp.stack([factor, local_tile.astype(jnp.float32)], axis=-1)
    arrived, info = (
        lax.all_to_all(picked, "tile", split_axis=0, concat_axis=0, tiled=True),
        lax.all_to_all(details, "tile", split_axis=0, concat_axis=0, tiled=True),
    )
    partial_image = refine_accumulate(
        arrived.reshape(-1, BX, plane), info.reshape(-1, 2), 2 * BX, group
    )
    return lax.psum_scatter(partial_image, "src", scatter_dimension=1, tiled=True)


YP = BY * BZ // LANES
HALO_LO = YP
HALO_HI = YP + 1
BLOCK = YP + 2


def cos_series():
    nodes = 400
    v = 0.125 + 0.125 * np.cos(np.pi * (np.arange(nodes) + 0.5) / nodes)
    cheb = np.polynomial.chebyshev.Chebyshev.fit(
        v, np.cos(2 * np.pi * np.sqrt(v)), 5, domain=[0.0, 0.25]
    )
    return [float(c) for c in cheb.convert(kind=np.polynomial.Polynomial, domain=[-1, 1]).coef]


def refine_columns():
    m = np.zeros((2 * BZ, BZ), np.float64)
    for i in range(2 * BZ):
        k = i // 2
        other = max(k - 1, 0) if i % 2 == 0 else min(k + 1, BZ - 1)
        m[i, k] += 0.75
        m[i, other] += 0.25
    out = np.zeros((2, 2, BZ, 2, 2, 2 * BZ), np.float64)
    for split in range(2):
        for scale, factor in enumerate((0.75, 0.25)):
            for parity in range(2):
                out[split, parity, :, scale, parity, :] = factor * m.T
    return out.reshape(4 * BZ, 8 * BZ)


def slot_scalars(mask_ref, weight_ref, first, group, slot):
    count = jnp.int32(0)
    local = jnp.int32(0)
    weight = jnp.float32(0.0)
    for i in range(group):
        live = mask_ref[0, first + i] == 1
        hit = jnp.logical_and(live, count == slot)
        local = jnp.where(hit, jnp.int32(i), local)
        weight = jnp.where(hit, weight_ref[0, first + i], weight)
        count = count + live.astype(jnp.int32)
    return local, weight


def put_halo(out_ref, where, row):
    for y in range(YP):
        out_ref[where + (pl.ds(y, 1), slice(None))] = row[:, y * LANES : (y + 1) * LANES]


def pick_kernel(quarters, owners, group, capacity, mask_ref, weight_ref, tables_ref, out_ref, buf, sem):
    def copy(g, j):
        local, _ = slot_scalars(mask_ref, weight_ref, g * group, group, j)
        return pltpu.make_async_copy(
            tables_ref.at[g * group + local], buf.at[g * capacity + j], sem.at[g * capacity + j]
        )

    for g in range(owners):
        for j in range(capacity):
            copy(g, j).start()
    rows = lax.broadcasted_iota(jnp.int32, (SUB, LANES), 0)
    lanes = lax.broadcasted_iota(jnp.int32, (SUB, LANES), 1)
    for g in range(owners):
        info = jnp.zeros((SUB, LANES), jnp.float32)
        for j in range(capacity):
            local, weight = slot_scalars(mask_ref, weight_ref, g * group, group, j)
            info = jnp.where(lanes == 2 * j, weight, info)
            info = jnp.where(lanes == 2 * j + 1, local.astype(jnp.float32), info)
        for q in range(quarters):
            out_ref[q * owners + g, capacity * BLOCK] = info
        for j in range(capacity):
            s = g * capacity + j
            copy(g, j).wait()
            for q in range(quarters):
                d = q * owners + g
                for y in range(YP):
                    out_ref[d, j * BLOCK + y] = buf[s, q, :, y * LANES : (y + 1) * LANES]
                lo = buf[s, q - 1, 7:8, :] if q > 0 else buf[s, 0, 0:1, :]
                hi = buf[s, q + 1, 0:1, :] if q < quarters - 1 else buf[s, q, 7:8, :]
                put_halo(out_ref, (d, j * BLOCK + HALO_LO), lo)
                put_halo(out_ref, (d, j * BLOCK + HALO_HI), hi)


def pick(tables, weights, aperture, quarters, owners, group, capacity):
    n = quarters * owners
    blocks = capacity * BLOCK + 1
    return pl.pallas_call(
        functools.partial(pick_kernel, quarters, owners, group, capacity),
        name="pick",
        out_shape=jax.ShapeDtypeStruct((n, blocks, SUB, LANES), jnp.float32),
        in_specs=[
            pl.BlockSpec(memory_space=pltpu.SMEM),
            pl.BlockSpec(memory_space=pltpu.SMEM),
            pl.BlockSpec(memory_space=pl.ANY),
        ],
        out_specs=pl.BlockSpec(memory_space=pltpu.VMEM),
        scratch_shapes=[
            pltpu.VMEM((owners * capacity, quarters, SUB, YP * LANES), jnp.float32),
            pltpu.SemaphoreType.DMA((owners * capacity,)),
        ],
    )(aperture, weights, tables.reshape(-1, quarters, SUB, YP * LANES))


def add_slot(acc_ref, series, block, low, high, columns, weight, tile):
    rows = lax.broadcasted_iota(jnp.int32, (SUB, LANES), 0)
    turns = angular_rate / (2 * math.pi)
    near, away = 0.75 * turns, 0.25 * turns
    even, odd = [], []
    for y in range(YP):
        c = block(y)
        down = jnp.where(rows == 0, jnp.broadcast_to(low(y), c.shape), pltpu.roll(c, 1, 0))
        up = jnp.where(rows == SUB - 1, jnp.broadcast_to(high(y), c.shape), pltpu.roll(c, SUB - 1, 0))
        mid = near * c
        even.append(mid + away * down)
        odd.append(mid + away * up)
    x = jnp.concatenate(even + odd, axis=0)
    top = x.astype(jnp.bfloat16)
    rest = (x - top.astype(jnp.float32)).astype(jnp.bfloat16)
    res = jnp.dot(jnp.concatenate([top, rest], axis=1), columns, preferred_element_type=jnp.float32)
    scaled = [weight * c for c in series]

    def part(parity, y, k):
        r = (parity * YP + y) * SUB
        return res[r : r + SUB, k * LANES : (k + 1) * LANES]

    for parity in range(2):
        for y in range(YP):
            te, to, he, ho = (part(parity, y, k) for k in range(4))
            before = part(parity, y - 1, 3) if y > 0 else he
            after = part(parity, y + 1, 2) if y < YP - 1 else ho
            for k, t in enumerate((te + before, te + ho, to + he, to + after)):
                r = t - jnp.round(t)
                u = r * r
                p = scaled[5]
                for c in scaled[4:0:-1]:
                    p = p * u + c
                where = (tile, parity, 4 * y + k)
                acc_ref[where] = acc_ref[where] + p * u


def image_kernel(step, capacity, series, tiles, in_ref, all_ref, columns_ref, out_ref, acc, info, bias, sem):
    i = pl.program_id(0)
    copy = pltpu.make_async_copy(all_ref.at[:, capacity * BLOCK, pl.ds(0, 1), :], info, sem)

    @pl.when(i == 0)
    def _():
        copy.start()
        acc[...] = jnp.zeros_like(acc)
        for t in range(tiles):
            bias[t] = jnp.float32(0.0)
        copy.wait()

    columns = columns_ref[...]

    def one(n, carry):
        for j in range(capacity):
            weight = info[i * step + n, 0, 2 * j]
            tile = info[i * step + n, 0, 2 * j + 1].astype(jnp.int32)
            bias[tile] = bias[tile] + weight * series[0]
            add_slot(
                acc,
                series,
                lambda y: in_ref[n, j * BLOCK + y],
                lambda y: in_ref[n, j * BLOCK + HALO_LO, pl.ds(y, 1), :],
                lambda y: in_ref[n, j * BLOCK + HALO_HI, pl.ds(y, 1), :],
                columns,
                weight,
                tile,
            )
        return carry

    lax.fori_loop(0, step, one, 0)

    @pl.when(i == pl.num_programs(0) - 1)
    def _():
        span = 2 * SUB * 2 * BY

        def flush(t, carry):
            for parity in range(2):
                for y in range(2 * BY):
                    start = t * span + parity * 2 * BY + y
                    out_ref[pl.ds(start, SUB, stride=4 * BY), :] = acc[t, parity, y] + bias[t]
            return carry

        lax.fori_loop(0, tiles, flush, 0)


def image_of(arrived, tiles, capacity):
    n, blocks = arrived.shape[:2]
    step = 4
    columns = jnp.asarray(refine_columns(), jnp.bfloat16)
    rows = tiles * 2 * SUB * 2 * BY
    return pl.pallas_call(
        functools.partial(image_kernel, step, capacity, cos_series(), tiles),
        name="image",
        grid=(n // step,),
        out_shape=jax.ShapeDtypeStruct((rows, LANES), jnp.float32),
        in_specs=[
            pl.BlockSpec((step, blocks, SUB, LANES), lambda i: (i, 0, 0, 0)),
            pl.BlockSpec(memory_space=pl.ANY),
            pl.BlockSpec(columns.shape, lambda i: (0, 0)),
        ],
        out_specs=pl.BlockSpec((rows, LANES), lambda i: (0, 0)),
        scratch_shapes=[
            pltpu.VMEM((tiles, 2, 2 * BY, SUB, LANES), jnp.float32),
            pltpu.SMEM((n, 1, LANES), jnp.float32),
            pltpu.SMEM((tiles,), jnp.float32),
            pltpu.SemaphoreType.DMA,
        ],
    )(arrived, arrived, columns)


def octet_shards(tables, weights, aperture):
    quarters, owners = lax.axis_size("src"), lax.axis_size("tile")
    group = tables.shape[1] // owners
    capacity = group // 2
    sent = pick(tables[0], weights, aperture, quarters, owners, group, capacity)
    arrived = lax.all_to_all(sent, ("src", "tile"), split_axis=0, concat_axis=0, tiled=True)
    image = image_of(arrived, group, capacity)
    return image.reshape(group, 2 * SUB, 2 * BY, 2 * BZ)


def solution(mesh):
    placed = (
        P(("src", "tile"), None, None, None),
        P(("src", "tile"), None),
        P(("src", "tile"), None),
    )
    fits = BX == mesh.shape["src"] * SUB
    return jax.shard_map(
        octet_shards if fits else general_shards,
        mesh=mesh,
        in_specs=placed,
        out_specs=P("tile", "src", None, None),
        check_vma=False,
    )
```

```python
import functools
import math

import jax
import jax.numpy as jnp
import numpy as np
from jax import lax
from jax.experimental import pallas as pl
from jax.experimental.pallas import tpu as pltpu
from jax.sharding import PartitionSpec as P


BX = 32
BY = 16
BZ = 64
SUB = 8
LANES = 128

angular_rate = 9.0


def refine_axis(values, axis):
    length = values.shape[axis]
    first = lax.slice_in_dim(values, 0, 1, axis=axis)
    last = lax.slice_in_dim(values, length - 1, length, axis=axis)
    lower = jnp.concatenate([first, lax.slice_in_dim(values, 0, length - 1, axis=axis)], axis=axis)
    upper = jnp.concatenate([lax.slice_in_dim(values, 1, length, axis=axis), last], axis=axis)
    even_rows = 0.75 * values + 0.25 * lower
    odd_rows = 0.75 * values + 0.25 * upper
    paired = jnp.stack([even_rows, odd_rows], axis=axis + 1)
    shape = values.shape[:axis] + (2 * length,) + values.shape[axis + 1 :]
    return paired.reshape(shape)


def refine_accumulate(coarse, details, fine_rows, tile_count):
    items = coarse.shape[0]
    turns = 8
    block = items // turns
    coarse_rows = coarse.shape[1]
    tile_ids = jnp.arange(tile_count).astype(jnp.float32)

    def one_block(total, item):
        bricks, info = item
        shaped = bricks.reshape(block, coarse_rows, BY, BZ)
        along_x = refine_axis(shaped, 1)
        along_z = refine_axis(along_x, 3)
        fine = refine_axis(along_z, 2)
        phase = jnp.cos(angular_rate * fine)
        select = (info[:, 1:2] == tile_ids[None, :]).astype(jnp.float32) * info[:, 0:1]
        total = total + jnp.einsum("kp,kfyz->pfyz", select, phase, precision=lax.Precision.HIGHEST)
        return (total, None)

    stacked = (
        coarse.reshape(turns, block, coarse_rows, coarse.shape[2]),
        details.reshape(turns, block, 2),
    )
    start = jnp.zeros((tile_count, fine_rows, 2 * BY, 2 * BZ), jnp.float32)
    total, _ = lax.scan(one_block, start, stacked)
    return total


def general_shards(tables, weights, aperture):
    bricks = tables[0]
    own_weight = weights[0]
    own_mask = aperture[0]
    owners = lax.axis_size("tile")
    group = bricks.shape[0] // owners
    capacity = group // 2
    plane = bricks.shape[2]
    live = own_mask.reshape(owners, group)
    ranking = jnp.cumsum(live, axis=1) - 1
    slot_ids = jnp.arange(capacity)
    chosen = ((live[:, None, :] == 1) & (ranking[:, None, :] == slot_ids[None, :, None])).astype(
        jnp.int32
    )
    local_tile = jnp.sum(chosen * jnp.arange(group)[None, None, :], axis=2)
    occupied = jnp.sum(chosen, axis=2)
    brick_index = local_tile + jnp.arange(owners)[:, None] * group
    picked = bricks[brick_index]
    factor = own_weight[brick_index] * occupied.astype(jnp.float32)
    details = jnp.stack([factor, local_tile.astype(jnp.float32)], axis=-1)
    arrived, info = (
        lax.all_to_all(picked, "tile", split_axis=0, concat_axis=0, tiled=True),
        lax.all_to_all(details, "tile", split_axis=0, concat_axis=0, tiled=True),
    )
    partial_image = refine_accumulate(
        arrived.reshape(-1, BX, plane), info.reshape(-1, 2), 2 * BX, group
    )
    return lax.psum_scatter(partial_image, "src", scatter_dimension=1, tiled=True)


YP = BY * BZ // LANES
BLOCK = YP + 2
SLOTS = 2
SIDE = SLOTS * BLOCK
MESSAGE = 2 * SIDE + 1
FINE = 2 * BY


def cos_series():
    nodes = 400
    v = 0.125 + 0.125 * np.cos(np.pi * (np.arange(nodes) + 0.5) / nodes)
    cheb = np.polynomial.chebyshev.Chebyshev.fit(
        v, np.cos(2 * np.pi * np.sqrt(v)), 5, domain=[0.0, 0.25]
    )
    return [float(c) for c in cheb.convert(kind=np.polynomial.Polynomial, domain=[-1, 1]).coef]


def refine_columns():
    m = np.zeros((2 * BZ, BZ), np.float64)
    for i in range(2 * BZ):
        k = i // 2
        other = max(k - 1, 0) if i % 2 == 0 else min(k + 1, BZ - 1)
        m[i, k] += 0.75
        m[i, other] += 0.25
    out = np.zeros((2, 2, BZ, 2, 2, 2 * BZ), np.float64)
    for split in range(2):
        for scale, factor in enumerate((0.75, 0.25)):
            for parity in range(2):
                out[split, parity, :, scale, parity, :] = factor * m.T
    return out.reshape(4 * BZ, 8 * BZ)


def slot_scalars(mask_ref, weight_ref, first, group, slot):
    count = jnp.int32(0)
    local = jnp.int32(0)
    weight = jnp.float32(0.0)
    for i in range(group):
        live = mask_ref[0, first + i] == 1
        hit = jnp.logical_and(live, count == slot)
        local = jnp.where(hit, jnp.int32(i), local)
        weight = jnp.where(hit, weight_ref[0, first + i], weight)
        count = count + live.astype(jnp.int32)
    return local, weight


def pick_kernel(sends, quarters, owners, group, mask_ref, weight_ref, tables_ref, *refs):
    outs, (buf, sem) = refs[: len(sends)], refs[len(sends) :]
    copies = []
    for g in range(owners):
        for j in range(SLOTS):
            local, _ = slot_scalars(mask_ref, weight_ref, g * group, group, j)
            s = g * SLOTS + j
            copy = pltpu.make_async_copy(tables_ref.at[g * group + local], buf.at[s], sem.at[s])
            copy.start()
            copies.append(copy)
    r, t = lax.axis_index("src"), lax.axis_index("tile")
    lanes = lax.broadcasted_iota(jnp.int32, (SUB, LANES), 1)
    for out_ref, (dz, dt) in zip(outs, sends):
        info = jnp.zeros((SUB, LANES), jnp.float32)
        for side in range(2):
            g = t ^ (dt ^ side)
            for j in range(SLOTS):
                local, weight = slot_scalars(mask_ref, weight_ref, g * group, group, j)
                lane = 2 * (side * SLOTS + j)
                info = jnp.where(lanes == lane, weight, info)
                info = jnp.where(lanes == lane + 1, local.astype(jnp.float32), info)
        out_ref[SIDE] = info
    for copy in copies:
        copy.wait()
    for out_ref, (dz, dt) in zip(outs, sends):
        q = r ^ dz
        below, above = jnp.maximum(q - 1, 0), jnp.minimum(q + 1, quarters - 1)
        for side in range(2):
            g = t ^ (dt ^ side)
            for j in range(SLOTS):
                s = g * SLOTS + j
                first = side * (SIDE + 1) + j * BLOCK
                for y in range(YP):
                    at = slice(y * LANES, (y + 1) * LANES)
                    out_ref[first + y] = buf[s, q, :, at]
                    out_ref[first + YP, y : y + 1, :] = jnp.where(
                        q > 0, buf[s, below, SUB - 1 : SUB, at], buf[s, below, 0:1, at]
                    )
                    out_ref[first + YP + 1, y : y + 1, :] = jnp.where(
                        q < quarters - 1, buf[s, above, 0:1, at], buf[s, above, SUB - 1 : SUB, at]
                    )


def pick(sends, bricks, weights, aperture, owners):
    group = bricks.shape[0] // owners
    quarters = bricks.shape[1]
    return pl.pallas_call(
        functools.partial(pick_kernel, sends, quarters, owners, group),
        out_shape=[pltpu.VMEM((MESSAGE, SUB, LANES), jnp.float32) for _ in sends],
        in_specs=[
            pl.BlockSpec(memory_space=pltpu.SMEM),
            pl.BlockSpec(memory_space=pltpu.SMEM),
            pl.BlockSpec(memory_space=pltpu.HBM),
        ],
        out_specs=[pl.BlockSpec(memory_space=pltpu.VMEM) for _ in sends],
        scratch_shapes=[
            pltpu.VMEM((owners * SLOTS,) + bricks.shape[1:], jnp.float32),
            pltpu.SemaphoreType.DMA((owners * SLOTS,)),
        ],
        compiler_params=pltpu.CompilerParams(vmem_limit_bytes=16 << 20),
    )(aperture, weights, pltpu.with_memory_space_constraint(bricks, pltpu.HBM))


def refine_side(ref, base, columns_ref, res_ref):
    rows = lax.broadcasted_iota(jnp.int32, (SUB, LANES), 0)
    turns = angular_rate / (2 * math.pi)
    near, away = 0.75 * turns, 0.25 * turns
    parts = []
    for j in range(SLOTS):
        even, odd = [], []
        for y in range(YP):
            first = base + j * BLOCK
            c = ref[first + y]
            low = jnp.broadcast_to(ref[first + YP, y : y + 1, :], c.shape)
            high = jnp.broadcast_to(ref[first + YP + 1, y : y + 1, :], c.shape)
            mid = near * c
            even.append(mid + away * jnp.where(rows == 0, low, pltpu.roll(c, 1, 0)))
            odd.append(mid + away * jnp.where(rows == SUB - 1, high, pltpu.roll(c, SUB - 1, 0)))
        parts += even + odd
    x = jnp.concatenate(parts, axis=0)
    top = x.astype(jnp.bfloat16)
    rest = (x - top.astype(jnp.float32)).astype(jnp.bfloat16)
    res_ref[...] = jnp.dot(
        jnp.concatenate([top, rest], axis=1), columns_ref[...], preferred_element_type=jnp.float32
    )


def add_slot(acc_ref, series, res_ref, j, weight, tile):
    scaled = [weight * c for c in series]
    for parity in range(2):

        def part(pair, k):
            r = ((j * 2 + parity) * YP + pair) * SUB
            return res_ref[r : r + SUB, k * LANES : (k + 1) * LANES]

        for y in range(FINE):
            pair, k = divmod(y, 4)
            if k == 0:
                t = part(pair, 0) + (part(pair - 1, 3) if pair > 0 else part(pair, 2))
            elif k == 1:
                t = part(pair, 0) + part(pair, 3)
            elif k == 2:
                t = part(pair, 1) + part(pair, 2)
            else:
                t = part(pair, 1) + (part(pair + 1, 2) if pair < YP - 1 else part(pair, 3))
            r = t - jnp.round(t)
            u = r * r
            p = scaled[5]
            for c in scaled[4:0:-1]:
                p = p * u + c
            acc_ref[tile, parity, y] = acc_ref[tile, parity, y] + p * u


def image_kernel(entries, rows, arrays, carried, sides, final, group, *refs):
    ins, columns_ref, refs = refs[:arrays], refs[arrays], refs[arrays + 1 :]
    old, refs = refs[:carried], refs[carried:]
    if final:
        out_ref, acc, refs = refs[0], refs[1:2], refs[2:]
    else:
        acc, refs = refs[:sides], refs[sides:]
    bias, info, sem, res = refs[0], refs[1], refs[2], refs[3:]
    copies = [
        pltpu.make_async_copy(ins[which].at[tile, pl.ds(0, 1), :], info.at[k], sem.at[k])
        for k, (which, tile) in enumerate(rows)
    ]
    for copy in copies:
        copy.start()
    series = cos_series()
    refine_side(ins[entries[0][0]], entries[0][1], columns_ref, res[0])
    for k in range(sides * group):
        bias[k] = jnp.float32(0.0)
    for copy in copies:
        copy.wait()

    def scalars(entry, j):
        weight = info[entry[2], 0, entry[3] + 2 * j]
        tile = info[entry[2], 0, entry[3] + 2 * j + 1].astype(jnp.int32)
        return weight, tile

    for entry in entries:
        for j in range(SLOTS):
            weight, tile = scalars(entry, j)
            k = entry[4] * group + tile
            bias[k] = bias[k] + weight * series[0]

    for side in range(sides):
        seeds = old if final else old[side : side + 1]

        def seed(k, carry):
            level = bias[side * group + k]
            for parity in range(2):
                for y in range(FINE):
                    value = jnp.full((SUB, LANES), level, jnp.float32)
                    for s in seeds:
                        value = value + s[k, parity, y]
                    acc[side][k, parity, y] = value
            return carry

        lax.fori_loop(0, group, seed, 0)

    for n, entry in enumerate(entries):
        if n + 1 < len(entries):
            later = entries[n + 1]
            refine_side(ins[later[0]], later[1], columns_ref, res[(n + 1) % 2])
        for j in range(SLOTS):
            weight, tile = scalars(entry, j)
            add_slot(acc[entry[4]], series, res[n % 2], j, weight, tile)

    if final:

        def flush(k, carry):
            for parity in range(2):
                for y in range(FINE):
                    start = k * (2 * SUB * FINE) + parity * FINE + y
                    out_ref[pl.ds(start, SUB, stride=2 * FINE), :] = acc[0][k, parity, y]
            return carry

        lax.fori_loop(0, group, flush, 0)


def image_step(messages, relayed, old, columns, group, final):
    sides = 1 if final else 2
    near = functools.partial(pltpu.with_memory_space_constraint, memory_space=pltpu.VMEM)
    entries, arrays, rows = [], [], []
    for m in messages:
        for side in range(sides):
            entries.append((len(arrays), side * (SIDE + 1), len(rows), side * 2 * SLOTS, side))
        rows.append((len(arrays), SIDE))
        arrays.append(m)
    if relayed is not None:
        for first in range(0, relayed.shape[0], SIDE + 1):
            entries.append((len(arrays), first + 1, len(rows), 2 * SLOTS, 0))
            rows.append((len(arrays), first))
        arrays.append(relayed)
    shape = (group, 2, FINE, SUB, LANES)
    whole = pl.BlockSpec(memory_space=pltpu.VMEM)
    scratch = [
        pltpu.SMEM((sides * group,), jnp.float32),
        pltpu.SMEM((len(rows), 1, LANES), jnp.float32),
        pltpu.SemaphoreType.DMA((len(rows),)),
        pltpu.VMEM((SLOTS * 2 * YP * SUB, 4 * LANES), jnp.float32),
        pltpu.VMEM((SLOTS * 2 * YP * SUB, 4 * LANES), jnp.float32),
    ]
    if final:
        out_shape = jax.ShapeDtypeStruct((group * 2 * SUB * FINE, LANES), jnp.float32)
        out_specs = whole
        scratch = [pltpu.VMEM(shape, jnp.float32)] + scratch
    else:
        out_shape = [pltpu.VMEM(shape, jnp.float32)] * 2
        out_specs = [whole] * 2
    return pl.pallas_call(
        functools.partial(
            image_kernel, entries, rows, len(arrays), len(old), sides, final, group
        ),
        out_shape=out_shape,
        in_specs=[whole] * (len(arrays) + 1 + len(old)),
        out_specs=out_specs,
        scratch_shapes=scratch,
        compiler_params=pltpu.CompilerParams(vmem_limit_bytes=16 << 20),
    )(*[near(a) for a in arrays], near(columns), *[near(a) for a in old])


def octet_shards(tables, weights, aperture):
    quarters, owners = lax.axis_size("src"), lax.axis_size("tile")
    group = tables.shape[1] // owners
    columns = jnp.asarray(refine_columns(), jnp.bfloat16)
    bricks = tables[0].reshape(-1, quarters, SUB, YP * LANES)

    def permute(value, dz, dt):
        def other(r, t):
            return (r ^ dz) * owners + (t ^ dt)

        pairs = [(r * owners + t, other(r, t)) for r in range(quarters) for t in range(owners)]
        return lax.ppermute(value, ("src", "tile"), pairs)

    chips = range(0, owners, 2)
    lead = [(2, 0), (3, 0)]
    near = [(0, dt) for dt in chips[1:]]
    far = [(dz, dt) for dz in (2, 3) for dt in chips[1:]]
    side = [(1, dt) for dt in chips]
    order = lead + near + far + side
    batches = [[(0, 0)] + near, lead + far[:2], far[2:], side[:-2], side[-2:]]
    got = {}
    sent = dict(zip(lead, pick(lead, bricks, weights, aperture, owners)))
    rest = [(0, 0)] + order[len(lead) :]
    sent.update(zip(rest, pick(rest, bricks, weights, aperture, owners)))
    got[0, 0] = sent[0, 0]
    for key in order:
        got[key] = permute(sent[key], *key)
    images = []
    for batch in batches[:-1]:
        messages = [got[key] for key in batch]
        images = image_step(messages, None, images, columns, group, False)
    mine, other = images
    late = [got[key] for key in batches[-1]]
    other = permute(other, 0, 1)
    relayed = permute(jnp.concatenate([m[SIDE:] for m in late], axis=0), 0, 1)
    image = image_step(late, relayed, [mine, other], columns, group, True)
    return image.reshape(group, 2 * SUB, FINE, 2 * BZ)


def solution(mesh):
    placed = (
        P(("src", "tile"), None, None, None),
        P(("src", "tile"), None),
        P(("src", "tile"), None),
    )
    quarters, owners = mesh.shape["src"], mesh.shape["tile"]
    fits = quarters == 4 and BX == quarters * SUB and owners == 8
    return jax.shard_map(
        octet_shards if fits else general_shards,
        mesh=mesh,
        in_specs=placed,
        out_specs=P("tile", "src", None, None),
        check_vma=False,
    )
```

```python
import functools
import math

import jax
import jax.numpy as jnp
import numpy as np
from jax import lax
from jax.experimental import pallas as pl
from jax.experimental.pallas import tpu as pltpu
from jax.sharding import PartitionSpec as P


BX = 32
BY = 16
BZ = 64
SUB = 8
LANES = 128

angular_rate = 9.0


def refine_axis(values, axis):
    length = values.shape[axis]
    first = lax.slice_in_dim(values, 0, 1, axis=axis)
    last = lax.slice_in_dim(values, length - 1, length, axis=axis)
    lower = jnp.concatenate([first, lax.slice_in_dim(values, 0, length - 1, axis=axis)], axis=axis)
    upper = jnp.concatenate([lax.slice_in_dim(values, 1, length, axis=axis), last], axis=axis)
    even_rows = 0.75 * values + 0.25 * lower
    odd_rows = 0.75 * values + 0.25 * upper
    paired = jnp.stack([even_rows, odd_rows], axis=axis + 1)
    shape = values.shape[:axis] + (2 * length,) + values.shape[axis + 1 :]
    return paired.reshape(shape)


def refine_accumulate(coarse, details, fine_rows, tile_count):
    items = coarse.shape[0]
    turns = 8
    block = items // turns
    coarse_rows = coarse.shape[1]
    tile_ids = jnp.arange(tile_count).astype(jnp.float32)

    def one_block(total, item):
        bricks, info = item
        shaped = bricks.reshape(block, coarse_rows, BY, BZ)
        along_x = refine_axis(shaped, 1)
        along_z = refine_axis(along_x, 3)
        fine = refine_axis(along_z, 2)
        phase = jnp.cos(angular_rate * fine)
        select = (info[:, 1:2] == tile_ids[None, :]).astype(jnp.float32) * info[:, 0:1]
        total = total + jnp.einsum("kp,kfyz->pfyz", select, phase, precision=lax.Precision.HIGHEST)
        return (total, None)

    stacked = (
        coarse.reshape(turns, block, coarse_rows, coarse.shape[2]),
        details.reshape(turns, block, 2),
    )
    start = jnp.zeros((tile_count, fine_rows, 2 * BY, 2 * BZ), jnp.float32)
    total, _ = lax.scan(one_block, start, stacked)
    return total


def general_shards(tables, weights, aperture):
    bricks = tables[0]
    own_weight = weights[0]
    own_mask = aperture[0]
    owners = lax.axis_size("tile")
    group = bricks.shape[0] // owners
    capacity = group // 2
    plane = bricks.shape[2]
    live = own_mask.reshape(owners, group)
    ranking = jnp.cumsum(live, axis=1) - 1
    slot_ids = jnp.arange(capacity)
    chosen = ((live[:, None, :] == 1) & (ranking[:, None, :] == slot_ids[None, :, None])).astype(
        jnp.int32
    )
    local_tile = jnp.sum(chosen * jnp.arange(group)[None, None, :], axis=2)
    occupied = jnp.sum(chosen, axis=2)
    brick_index = local_tile + jnp.arange(owners)[:, None] * group
    picked = bricks[brick_index]
    factor = own_weight[brick_index] * occupied.astype(jnp.float32)
    details = jnp.stack([factor, local_tile.astype(jnp.float32)], axis=-1)
    arrived, info = (
        lax.all_to_all(picked, "tile", split_axis=0, concat_axis=0, tiled=True),
        lax.all_to_all(details, "tile", split_axis=0, concat_axis=0, tiled=True),
    )
    partial_image = refine_accumulate(
        arrived.reshape(-1, BX, plane), info.reshape(-1, 2), 2 * BX, group
    )
    return lax.psum_scatter(partial_image, "src", scatter_dimension=1, tiled=True)


YP = BY * BZ // LANES
BLOCK = YP + 2
SLOTS = 2
SIDE = SLOTS * BLOCK
MESSAGE = 2 * SIDE + 1
FINE = 2 * BY


def cos_series():
    nodes = 400
    v = 0.125 + 0.125 * np.cos(np.pi * (np.arange(nodes) + 0.5) / nodes)
    cheb = np.polynomial.chebyshev.Chebyshev.fit(
        v, np.cos(2 * np.pi * np.sqrt(v)), 5, domain=[0.0, 0.25]
    )
    return [float(c) for c in cheb.convert(kind=np.polynomial.Polynomial, domain=[-1, 1]).coef]


def refine_columns():
    m = np.zeros((2 * BZ, BZ), np.float64)
    for i in range(2 * BZ):
        k = i // 2
        other = max(k - 1, 0) if i % 2 == 0 else min(k + 1, BZ - 1)
        m[i, k] += 0.75
        m[i, other] += 0.25
    out = np.zeros((2, 2, BZ, 2, 2, 2 * BZ), np.float64)
    for split in range(2):
        for scale, factor in enumerate((0.75, 0.25)):
            for parity in range(2):
                out[split, parity, :, scale, parity, :] = factor * m.T
    return out.reshape(4 * BZ, 8 * BZ)


def slot_scalars(mask_ref, weight_ref, first, group, slot):
    count = jnp.int32(0)
    local = jnp.int32(0)
    weight = jnp.float32(0.0)
    for i in range(group):
        live = mask_ref[0, first + i] == 1
        hit = jnp.logical_and(live, count == slot)
        local = jnp.where(hit, jnp.int32(i), local)
        weight = jnp.where(hit, weight_ref[0, first + i], weight)
        count = count + live.astype(jnp.int32)
    return local, weight


def pick_kernel(sends, quarters, group, mask_in, weight_in, tables_ref, *refs):
    outs, (mask_ref, weight_ref, small, buf, sem) = refs[: len(sends)], refs[len(sends) :]
    heads = [
        pltpu.make_async_copy(mask_in, mask_ref, small.at[0]),
        pltpu.make_async_copy(weight_in, weight_ref, small.at[1]),
    ]
    for head in heads:
        head.start()
    for head in heads:
        head.wait()
    r, t = lax.axis_index("src"), lax.axis_index("tile")
    lanes = lax.broadcasted_iota(jnp.int32, (SUB, LANES), 1)
    offsets = sorted({dt ^ side for _, dt in sends for side in range(2)})
    found, copies = {}, []
    for n, offset in enumerate(offsets):
        g = t ^ offset
        for j in range(SLOTS):
            local, weight = slot_scalars(mask_ref, weight_ref, g * group, group, j)
            found[offset, j] = (n * SLOTS + j, local, weight)
            s = n * SLOTS + j
            copy = pltpu.make_async_copy(tables_ref.at[g * group + local], buf.at[s], sem.at[s])
            copy.start()
            copies.append(copy)
    for out_ref, (dz, dt) in zip(outs, sends):
        info = jnp.zeros((SUB, LANES), jnp.float32)
        for side in range(2):
            for j in range(SLOTS):
                _, local, weight = found[dt ^ side, j]
                lane = 2 * (side * SLOTS + j)
                info = jnp.where(lanes == lane, weight, info)
                info = jnp.where(lanes == lane + 1, local.astype(jnp.float32), info)
        out_ref[SIDE] = info
    for copy in copies:
        copy.wait()
    for out_ref, (dz, dt) in zip(outs, sends):
        q = r ^ dz
        below, above = jnp.maximum(q - 1, 0), jnp.minimum(q + 1, quarters - 1)
        for side in range(2):
            for j in range(SLOTS):
                s = found[dt ^ side, j][0]
                first = side * (SIDE + 1) + j * BLOCK
                for y in range(YP):
                    at = slice(y * LANES, (y + 1) * LANES)
                    out_ref[first + y] = buf[s, q, :, at]
                    out_ref[first + YP, y : y + 1, :] = jnp.where(
                        q > 0, buf[s, below, SUB - 1 : SUB, at], buf[s, below, 0:1, at]
                    )
                    out_ref[first + YP + 1, y : y + 1, :] = jnp.where(
                        q < quarters - 1, buf[s, above, 0:1, at], buf[s, above, SUB - 1 : SUB, at]
                    )


def pick(sends, bricks, weights, aperture, owners):
    group = bricks.shape[0] // owners
    quarters = bricks.shape[1]
    slots = SLOTS * len({dt ^ side for _, dt in sends for side in range(2)})
    home = functools.partial(pltpu.with_memory_space_constraint, memory_space=pltpu.HBM)
    return pl.pallas_call(
        functools.partial(pick_kernel, sends, quarters, group),
        out_shape=[pltpu.VMEM((MESSAGE, SUB, LANES), jnp.float32) for _ in sends],
        in_specs=[pl.BlockSpec(memory_space=pltpu.HBM)] * 3,
        out_specs=[pl.BlockSpec(memory_space=pltpu.VMEM) for _ in sends],
        scratch_shapes=[
            pltpu.SMEM(aperture.shape, aperture.dtype),
            pltpu.SMEM(weights.shape, weights.dtype),
            pltpu.SemaphoreType.DMA((2,)),
            pltpu.VMEM((slots,) + bricks.shape[1:], jnp.float32),
            pltpu.SemaphoreType.DMA((slots,)),
        ],
        compiler_params=pltpu.CompilerParams(vmem_limit_bytes=16 << 20),
    )(home(aperture), home(weights), home(bricks))


def refine_side(ref, base, columns_ref, res_ref):
    rows = lax.broadcasted_iota(jnp.int32, (SUB, LANES), 0)
    turns = angular_rate / (2 * math.pi)
    near, away = 0.75 * turns, 0.25 * turns
    parts = []
    for j in range(SLOTS):
        even, odd = [], []
        for y in range(YP):
            first = base + j * BLOCK
            c = ref[first + y]
            low = jnp.broadcast_to(ref[first + YP, y : y + 1, :], c.shape)
            high = jnp.broadcast_to(ref[first + YP + 1, y : y + 1, :], c.shape)
            mid = near * c
            even.append(mid + away * jnp.where(rows == 0, low, pltpu.roll(c, 1, 0)))
            odd.append(mid + away * jnp.where(rows == SUB - 1, high, pltpu.roll(c, SUB - 1, 0)))
        parts += even + odd
    x = jnp.concatenate(parts, axis=0)
    top = x.astype(jnp.bfloat16)
    rest = (x - top.astype(jnp.float32)).astype(jnp.bfloat16)
    res_ref[...] = jnp.dot(
        jnp.concatenate([top, rest], axis=1), columns_ref[...], preferred_element_type=jnp.float32
    )


def add_slot(acc_ref, series, res_ref, j, weight, tile):
    scaled = [weight * c for c in series]
    for parity in range(2):

        def part(pair, k):
            r = ((j * 2 + parity) * YP + pair) * SUB
            return res_ref[r : r + SUB, k * LANES : (k + 1) * LANES]

        for y in range(FINE):
            pair, k = divmod(y, 4)
            if k == 0:
                t = part(pair, 0) + (part(pair - 1, 3) if pair > 0 else part(pair, 2))
            elif k == 1:
                t = part(pair, 0) + part(pair, 3)
            elif k == 2:
                t = part(pair, 1) + part(pair, 2)
            else:
                t = part(pair, 1) + (part(pair + 1, 2) if pair < YP - 1 else part(pair, 3))
            r = t - jnp.round(t)
            u = r * r
            p = scaled[5]
            for c in scaled[4::-1]:
                p = p * u + c
            at = slice((parity * FINE + y) * SUB, (parity * FINE + y + 1) * SUB)
            acc_ref[tile, at, :] = acc_ref[tile, at, :] + p


def image_kernel(entries, rows, arrays, sides, first, final, group, *refs):
    ins, columns_ref, refs = refs[:arrays], refs[arrays], refs[arrays + 1 :]
    if final:
        other_ref, refs = refs[1], refs[2:]
        out_ref, acc, refs = refs[0], refs[1:2], refs[2:]
        stage, out_sem, refs = refs[0], refs[1], refs[2:]
    else:
        refs = refs if first else refs[sides:]
        acc, refs = refs[:sides], refs[sides:]
    info, sem, res = refs[0], refs[1], refs[2:]
    copies = [
        pltpu.make_async_copy(ins[which].at[tile, pl.ds(0, 1), :], info.at[k], sem.at[k])
        for k, (which, tile) in enumerate(rows)
    ]
    for copy in copies:
        copy.start()
    series = cos_series()
    refine_side(ins[entries[0][0]], entries[0][1], columns_ref, res[0])
    if first:
        for image in acc:

            def clear(k, carry):
                image[k] = jnp.zeros(image.shape[1:], jnp.float32)
                return carry

            lax.fori_loop(0, group, clear, 0)
    for copy in copies:
        copy.wait()
    for n, entry in enumerate(entries):
        if n + 1 < len(entries):
            later = entries[n + 1]
            refine_side(ins[later[0]], later[1], columns_ref, res[(n + 1) % 2])
        for j in range(SLOTS):
            weight = info[entry[2], 0, entry[3] + 2 * j]
            tile = info[entry[2], 0, entry[3] + 2 * j + 1].astype(jnp.int32)
            add_slot(acc[entry[4]], series, res[n % 2], j, weight, tile)

    if final:
        written = []
        for k in range(group):
            for parity in range(2):
                for x in range(SUB):
                    for y in range(0, FINE, SUB):
                        at = pl.ds((parity * FINE + y) * SUB + x, SUB, stride=SUB)
                        row = (2 * x + parity) * FINE + y
                        stage[k, row : row + SUB, :] = acc[0][k, at, :] + other_ref[k, at, :]
            copy = pltpu.make_async_copy(stage.at[k], out_ref.at[k], out_sem.at[k])
            copy.start()
            written.append(copy)
        for copy in written:
            copy.wait()


def image_step(messages, relayed, images, columns, group, final=False, sides=2):
    near = functools.partial(pltpu.with_memory_space_constraint, memory_space=pltpu.VMEM)
    entries, arrays, rows = [], [], []
    for m in messages:
        for side in range(sides):
            entries.append((len(arrays), side * (SIDE + 1), len(rows), side * 2 * SLOTS, side))
        rows.append((len(arrays), SIDE))
        arrays.append(m)
    if relayed is not None:
        for first in range(0, relayed.shape[0], SIDE + 1):
            entries.append((len(arrays), first + 1, len(rows), 2 * SLOTS, 0))
            rows.append((len(arrays), first))
        arrays.append(relayed)
    shape = (group, 2 * FINE * SUB, LANES)
    whole = pl.BlockSpec(memory_space=pltpu.VMEM)
    scratch = [
        pltpu.SMEM((len(rows), 1, LANES), jnp.float32),
        pltpu.SemaphoreType.DMA((len(rows),)),
        pltpu.VMEM((SLOTS * 2 * YP * SUB, 4 * LANES), jnp.float32),
        pltpu.VMEM((SLOTS * 2 * YP * SUB, 4 * LANES), jnp.float32),
    ]
    kept = len(arrays) + 1
    if final:
        out_shape = [jax.ShapeDtypeStruct(shape, jnp.float32), pltpu.VMEM(shape, jnp.float32)]
        out_specs = [pl.BlockSpec(memory_space=pltpu.HBM), whole]
        scratch = [pltpu.VMEM(shape, jnp.float32), pltpu.SemaphoreType.DMA((group,))] + scratch
        aliases = {kept: 1}
    else:
        out_shape = [pltpu.VMEM(shape, jnp.float32)] * sides
        out_specs = [whole] * sides
        aliases = {kept + k: k for k in range(len(images))}
    return pl.pallas_call(
        functools.partial(
            image_kernel, entries, rows, len(arrays), sides, not images, final, group
        ),
        out_shape=out_shape,
        in_specs=[whole] * (kept + len(images)),
        out_specs=out_specs,
        scratch_shapes=scratch,
        input_output_aliases=aliases,
        compiler_params=pltpu.CompilerParams(vmem_limit_bytes=16 << 20),
    )(*[near(a) for a in arrays], near(columns), *[near(a) for a in images])


def octet_shards(tables, weights, aperture):
    quarters, owners = lax.axis_size("src"), lax.axis_size("tile")
    group = tables.shape[1] // owners
    columns = jnp.asarray(refine_columns(), jnp.bfloat16)
    bricks = tables[0].reshape(-1, quarters, SUB, YP * LANES)

    def permute(value, dz, dt):
        def other(r, t):
            return (r ^ dz) * owners + (t ^ dt)

        pairs = [(r * owners + t, other(r, t)) for r in range(quarters) for t in range(owners)]
        return lax.ppermute(value, ("src", "tile"), pairs)

    chips = range(0, owners, 2)
    lead = [(2, 0), (3, 0)]
    near = [(0, dt) for dt in chips[1:]]
    far = [(dz, dt) for dz in (2, 3) for dt in chips[1:]]
    side = [(1, dt) for dt in chips]
    order = lead + near + far + side
    batches = [
        [(0, 0)] + near,
        lead,
        [(2, 2), (2, 4)],
        [(2, 6), (3, 2)],
        [(1, 0), (1, 2)],
        [(3, 4), (1, 4)],
    ]
    last = [(3, 6), (1, 6)]
    got = {}
    sent = dict(zip(lead, pick(lead, bricks, weights, aperture, owners)))
    rest = [(0, 0)] + order[len(lead) :]
    sent.update(zip(rest, pick(rest, bricks, weights, aperture, owners)))
    got[0, 0] = sent[0, 0]
    for key in order:
        got[key] = permute(sent[key], *key)
    images = []
    for batch in batches:
        messages = [got[key] for key in batch]
        images = image_step(messages, None, images, columns, group)
    mine, other = images
    late = [got[key] for key in last]
    other = permute(other, 0, 1)
    relayed = permute(jnp.concatenate([m[SIDE:] for m in late], axis=0), 0, 1)
    (mine,) = image_step(late, None, [mine], columns, group, sides=1)
    image, _ = image_step([], relayed, [mine, other], columns, group, final=True, sides=1)
    return image.reshape(group, 2 * SUB, FINE, 2 * BZ)


def solution(mesh):
    placed = (
        P(("src", "tile"), None, None, None),
        P(("src", "tile"), None),
        P(("src", "tile"), None),
    )
    quarters, owners = mesh.shape["src"], mesh.shape["tile"]
    fits = quarters == 4 and BX == quarters * SUB and owners == 8
    return jax.shard_map(
        octet_shards if fits else general_shards,
        mesh=mesh,
        in_specs=placed,
        out_specs=P("tile", "src", None, None),
        check_vma=False,
    )
```

```python
import functools
import math

import jax
import jax.numpy as jnp
import numpy as np
from jax import lax
from jax.experimental import pallas as pl
from jax.experimental.pallas import tpu as pltpu
from jax.sharding import PartitionSpec as P


BX = 32
BY = 16
BZ = 64
SUB = 8
LANES = 128

angular_rate = 9.0


def refine_axis(values, axis):
    length = values.shape[axis]
    first = lax.slice_in_dim(values, 0, 1, axis=axis)
    last = lax.slice_in_dim(values, length - 1, length, axis=axis)
    lower = jnp.concatenate([first, lax.slice_in_dim(values, 0, length - 1, axis=axis)], axis=axis)
    upper = jnp.concatenate([lax.slice_in_dim(values, 1, length, axis=axis), last], axis=axis)
    even_rows = 0.75 * values + 0.25 * lower
    odd_rows = 0.75 * values + 0.25 * upper
    paired = jnp.stack([even_rows, odd_rows], axis=axis + 1)
    shape = values.shape[:axis] + (2 * length,) + values.shape[axis + 1 :]
    return paired.reshape(shape)


def refine_accumulate(coarse, details, fine_rows, tile_count):
    items = coarse.shape[0]
    turns = 8
    block = items // turns
    coarse_rows = coarse.shape[1]
    tile_ids = jnp.arange(tile_count).astype(jnp.float32)

    def one_block(total, item):
        bricks, info = item
        shaped = bricks.reshape(block, coarse_rows, BY, BZ)
        along_x = refine_axis(shaped, 1)
        along_z = refine_axis(along_x, 3)
        fine = refine_axis(along_z, 2)
        phase = jnp.cos(angular_rate * fine)
        select = (info[:, 1:2] == tile_ids[None, :]).astype(jnp.float32) * info[:, 0:1]
        total = total + jnp.einsum("kp,kfyz->pfyz", select, phase, precision=lax.Precision.HIGHEST)
        return (total, None)

    stacked = (
        coarse.reshape(turns, block, coarse_rows, coarse.shape[2]),
        details.reshape(turns, block, 2),
    )
    start = jnp.zeros((tile_count, fine_rows, 2 * BY, 2 * BZ), jnp.float32)
    total, _ = lax.scan(one_block, start, stacked)
    return total


def general_shards(tables, weights, aperture):
    bricks = tables[0]
    own_weight = weights[0]
    own_mask = aperture[0]
    owners = lax.axis_size("tile")
    group = bricks.shape[0] // owners
    capacity = group // 2
    plane = bricks.shape[2]
    live = own_mask.reshape(owners, group)
    ranking = jnp.cumsum(live, axis=1) - 1
    slot_ids = jnp.arange(capacity)
    chosen = ((live[:, None, :] == 1) & (ranking[:, None, :] == slot_ids[None, :, None])).astype(
        jnp.int32
    )
    local_tile = jnp.sum(chosen * jnp.arange(group)[None, None, :], axis=2)
    occupied = jnp.sum(chosen, axis=2)
    brick_index = local_tile + jnp.arange(owners)[:, None] * group
    picked = bricks[brick_index]
    factor = own_weight[brick_index] * occupied.astype(jnp.float32)
    details = jnp.stack([factor, local_tile.astype(jnp.float32)], axis=-1)
    arrived, info = (
        lax.all_to_all(picked, "tile", split_axis=0, concat_axis=0, tiled=True),
        lax.all_to_all(details, "tile", split_axis=0, concat_axis=0, tiled=True),
    )
    partial_image = refine_accumulate(
        arrived.reshape(-1, BX, plane), info.reshape(-1, 2), 2 * BX, group
    )
    return lax.psum_scatter(partial_image, "src", scatter_dimension=1, tiled=True)


YP = BY * BZ // LANES
BLOCK = YP + 2
SLOTS = 2
SIDE = SLOTS * BLOCK
MESSAGE = 2 * SIDE + 1
FINE = 2 * BY


def cos_series():
    nodes = 400
    v = 0.125 + 0.125 * np.cos(np.pi * (np.arange(nodes) + 0.5) / nodes)
    cheb = np.polynomial.chebyshev.Chebyshev.fit(
        v, np.cos(2 * np.pi * np.sqrt(v)), 5, domain=[0.0, 0.25]
    )
    return [float(c) for c in cheb.convert(kind=np.polynomial.Polynomial, domain=[-1, 1]).coef]


def refine_columns():
    m = np.zeros((2 * BZ, BZ), np.float64)
    for i in range(2 * BZ):
        k = i // 2
        other = max(k - 1, 0) if i % 2 == 0 else min(k + 1, BZ - 1)
        m[i, k] += 0.75
        m[i, other] += 0.25
    out = np.zeros((2, 2, BZ, 2, 2, 2 * BZ), np.float64)
    for split in range(2):
        for scale, factor in enumerate((0.75, 0.25)):
            for parity in range(2):
                out[split, parity, :, scale, parity, :] = factor * m.T
    return out.reshape(4 * BZ, 8 * BZ)


def slot_scalars(mask_ref, weight_ref, first, group, slot):
    count = jnp.int32(0)
    local = jnp.int32(0)
    weight = jnp.float32(0.0)
    for i in range(group):
        live = mask_ref[0, first + i] == 1
        hit = jnp.logical_and(live, count == slot)
        local = jnp.where(hit, jnp.int32(i), local)
        weight = jnp.where(hit, weight_ref[0, first + i], weight)
        count = count + live.astype(jnp.int32)
    return local, weight


def pick_kernel(sends, quarters, group, mask_in, weight_in, tables_ref, *refs):
    outs, (mask_ref, weight_ref, small, buf, sem) = refs[: len(sends)], refs[len(sends) :]
    heads = [
        pltpu.make_async_copy(mask_in, mask_ref, small.at[0]),
        pltpu.make_async_copy(weight_in, weight_ref, small.at[1]),
    ]
    for head in heads:
        head.start()
    r, t = lax.axis_index("src"), lax.axis_index("tile")
    offsets = sorted({dt ^ side for _, dt in sends for side in range(2)})
    ahead = buf.shape[0] == len(offsets) * group
    copies = []
    if ahead:
        for n, offset in enumerate(offsets):
            for i in range(group):
                s = n * group + i
                copy = pltpu.make_async_copy(
                    tables_ref.at[(t ^ offset) * group + i], buf.at[s], sem.at[s]
                )
                copy.start()
                copies.append(copy)
    for head in heads:
        head.wait()
    lanes = lax.broadcasted_iota(jnp.int32, (SUB, LANES), 1)
    found = {}
    for n, offset in enumerate(offsets):
        g = t ^ offset
        for j in range(SLOTS):
            local, weight = slot_scalars(mask_ref, weight_ref, g * group, group, j)
            if ahead:
                found[offset, j] = (n * group + local, local, weight)
                continue
            s = n * SLOTS + j
            found[offset, j] = (s, local, weight)
            copy = pltpu.make_async_copy(tables_ref.at[g * group + local], buf.at[s], sem.at[s])
            copy.start()
            copies.append(copy)
    for out_ref, (dz, dt) in zip(outs, sends):
        info = jnp.zeros((SUB, LANES), jnp.float32)
        for side in range(2):
            for j in range(SLOTS):
                _, local, weight = found[dt ^ side, j]
                lane = 2 * (side * SLOTS + j)
                info = jnp.where(lanes == lane, weight, info)
                info = jnp.where(lanes == lane + 1, local.astype(jnp.float32), info)
        out_ref[SIDE] = info
    for copy in copies:
        copy.wait()
    for out_ref, (dz, dt) in zip(outs, sends):
        q = r ^ dz
        below, above = jnp.maximum(q - 1, 0), jnp.minimum(q + 1, quarters - 1)
        for side in range(2):
            for j in range(SLOTS):
                s = found[dt ^ side, j][0]
                first = side * (SIDE + 1) + j * BLOCK
                for y in range(YP):
                    at = slice(y * LANES, (y + 1) * LANES)
                    out_ref[first + y] = buf[s, q, :, at]
                    out_ref[first + YP, y : y + 1, :] = jnp.where(
                        q > 0, buf[s, below, SUB - 1 : SUB, at], buf[s, below, 0:1, at]
                    )
                    out_ref[first + YP + 1, y : y + 1, :] = jnp.where(
                        q < quarters - 1, buf[s, above, 0:1, at], buf[s, above, SUB - 1 : SUB, at]
                    )


def pick(sends, bricks, weights, aperture, owners):
    group = bricks.shape[0] // owners
    quarters = bricks.shape[1]
    needed = len({dt ^ side for _, dt in sends for side in range(2)})
    slots = needed * (group if needed == 2 else SLOTS)
    home = functools.partial(pltpu.with_memory_space_constraint, memory_space=pltpu.HBM)
    return pl.pallas_call(
        functools.partial(pick_kernel, sends, quarters, group),
        out_shape=[pltpu.VMEM((MESSAGE, SUB, LANES), jnp.float32) for _ in sends],
        in_specs=[pl.BlockSpec(memory_space=pltpu.HBM)] * 3,
        out_specs=[pl.BlockSpec(memory_space=pltpu.VMEM) for _ in sends],
        scratch_shapes=[
            pltpu.SMEM(aperture.shape, aperture.dtype),
            pltpu.SMEM(weights.shape, weights.dtype),
            pltpu.SemaphoreType.DMA((2,)),
            pltpu.VMEM((slots,) + bricks.shape[1:], jnp.float32),
            pltpu.SemaphoreType.DMA((slots,)),
        ],
        compiler_params=pltpu.CompilerParams(vmem_limit_bytes=16 << 20),
    )(home(aperture), home(weights), home(bricks))


def refine_side(ref, base, columns_ref, res_ref):
    rows = lax.broadcasted_iota(jnp.int32, (SUB, LANES), 0)
    turns = angular_rate / (2 * math.pi)
    near, away = 0.75 * turns, 0.25 * turns
    parts = []
    for j in range(SLOTS):
        even, odd = [], []
        for y in range(YP):
            first = base + j * BLOCK
            c = ref[first + y]
            low = jnp.broadcast_to(ref[first + YP, y : y + 1, :], c.shape)
            high = jnp.broadcast_to(ref[first + YP + 1, y : y + 1, :], c.shape)
            mid = near * c
            even.append(mid + away * jnp.where(rows == 0, low, pltpu.roll(c, 1, 0)))
            odd.append(mid + away * jnp.where(rows == SUB - 1, high, pltpu.roll(c, SUB - 1, 0)))
        parts += even + odd
    x = jnp.concatenate(parts, axis=0)
    top = x.astype(jnp.bfloat16)
    rest = (x - top.astype(jnp.float32)).astype(jnp.bfloat16)
    res_ref[...] = jnp.dot(
        jnp.concatenate([top, rest], axis=1), columns_ref[...], preferred_element_type=jnp.float32
    )


def add_slot(acc_ref, series, res_ref, j, weight, tile):
    scaled = [weight * c for c in series]
    for parity in range(2):

        def part(pair, k):
            r = ((j * 2 + parity) * YP + pair) * SUB
            return res_ref[r : r + SUB, k * LANES : (k + 1) * LANES]

        for y in range(FINE):
            pair, k = divmod(y, 4)
            if k == 0:
                t = part(pair, 0) + (part(pair - 1, 3) if pair > 0 else part(pair, 2))
            elif k == 1:
                t = part(pair, 0) + part(pair, 3)
            elif k == 2:
                t = part(pair, 1) + part(pair, 2)
            else:
                t = part(pair, 1) + (part(pair + 1, 2) if pair < YP - 1 else part(pair, 3))
            r = t - jnp.round(t)
            u = r * r
            p = scaled[5]
            for c in scaled[4::-1]:
                p = p * u + c
            at = slice((parity * FINE + y) * SUB, (parity * FINE + y + 1) * SUB)
            acc_ref[tile, at, :] = acc_ref[tile, at, :] + p


def image_kernel(entries, rows, arrays, sides, first, final, group, *refs):
    ins, columns_ref, refs = refs[:arrays], refs[arrays], refs[arrays + 1 :]
    if final:
        other_ref, refs = refs[1], refs[2:]
        out_ref, acc, refs = refs[0], refs[1:2], refs[2:]
        stage, out_sem, refs = refs[0], refs[1], refs[2:]
    else:
        refs = refs if first else refs[sides:]
        acc, refs = refs[:sides], refs[sides:]
    info, sem, res = refs[0], refs[1], refs[2:]
    copies = [
        pltpu.make_async_copy(ins[which].at[tile, pl.ds(0, 1), :], info.at[k], sem.at[k])
        for k, (which, tile) in enumerate(rows)
    ]
    for copy in copies:
        copy.start()
    series = cos_series()
    refine_side(ins[entries[0][0]], entries[0][1], columns_ref, res[0])
    if first:
        for image in acc:

            def clear(k, carry):
                image[k] = jnp.zeros(image.shape[1:], jnp.float32)
                return carry

            lax.fori_loop(0, group, clear, 0)
    for copy in copies:
        copy.wait()
    for n, entry in enumerate(entries):
        if n + 1 < len(entries):
            later = entries[n + 1]
            refine_side(ins[later[0]], later[1], columns_ref, res[(n + 1) % 2])
        for j in range(SLOTS):
            weight = info[entry[2], 0, entry[3] + 2 * j]
            tile = info[entry[2], 0, entry[3] + 2 * j + 1].astype(jnp.int32)
            add_slot(acc[entry[4]], series, res[n % 2], j, weight, tile)

    if final:
        written = []
        for k in range(group):
            for parity in range(2):
                for x in range(SUB):
                    for y in range(0, FINE, SUB):
                        at = pl.ds((parity * FINE + y) * SUB + x, SUB, stride=SUB)
                        row = (2 * x + parity) * FINE + y
                        stage[k, row : row + SUB, :] = acc[0][k, at, :] + other_ref[k, at, :]
            copy = pltpu.make_async_copy(stage.at[k], out_ref.at[k], out_sem.at[k])
            copy.start()
            written.append(copy)
        for copy in written:
            copy.wait()


def image_step(messages, relayed, images, columns, group, final=False, sides=2):
    near = functools.partial(pltpu.with_memory_space_constraint, memory_space=pltpu.VMEM)
    entries, arrays, rows = [], [], []
    for m in messages:
        for side in range(sides):
            entries.append((len(arrays), side * (SIDE + 1), len(rows), side * 2 * SLOTS, side))
        rows.append((len(arrays), SIDE))
        arrays.append(m)
    if relayed is not None:
        for first in range(0, relayed.shape[0], SIDE + 1):
            entries.append((len(arrays), first + 1, len(rows), 2 * SLOTS, 0))
            rows.append((len(arrays), first))
        arrays.append(relayed)
    shape = (group, 2 * FINE * SUB, LANES)
    whole = pl.BlockSpec(memory_space=pltpu.VMEM)
    scratch = [
        pltpu.SMEM((len(rows), 1, LANES), jnp.float32),
        pltpu.SemaphoreType.DMA((len(rows),)),
        pltpu.VMEM((SLOTS * 2 * YP * SUB, 4 * LANES), jnp.float32),
        pltpu.VMEM((SLOTS * 2 * YP * SUB, 4 * LANES), jnp.float32),
    ]
    kept = len(arrays) + 1
    if final:
        out_shape = [jax.ShapeDtypeStruct(shape, jnp.float32), pltpu.VMEM(shape, jnp.float32)]
        out_specs = [pl.BlockSpec(memory_space=pltpu.HBM), whole]
        scratch = [pltpu.VMEM(shape, jnp.float32), pltpu.SemaphoreType.DMA((group,))] + scratch
        aliases = {kept: 1}
    else:
        out_shape = [pltpu.VMEM(shape, jnp.float32)] * sides
        out_specs = [whole] * sides
        aliases = {kept + k: k for k in range(len(images))}
    return pl.pallas_call(
        functools.partial(
            image_kernel, entries, rows, len(arrays), sides, not images, final, group
        ),
        out_shape=out_shape,
        in_specs=[whole] * (kept + len(images)),
        out_specs=out_specs,
        scratch_shapes=scratch,
        input_output_aliases=aliases,
        compiler_params=pltpu.CompilerParams(vmem_limit_bytes=16 << 20),
    )(*[near(a) for a in arrays], near(columns), *[near(a) for a in images])


def octet_shards(tables, weights, aperture):
    quarters, owners = lax.axis_size("src"), lax.axis_size("tile")
    group = tables.shape[1] // owners
    columns = jnp.asarray(refine_columns(), jnp.bfloat16)
    bricks = tables[0].reshape(-1, quarters, SUB, YP * LANES)

    def permute(value, dz, dt):
        def other(r, t):
            return (r ^ dz) * owners + (t ^ dt)

        pairs = [(r * owners + t, other(r, t)) for r in range(quarters) for t in range(owners)]
        return lax.ppermute(value, ("src", "tile"), pairs)

    chips = range(0, owners, 2)
    lead = [(2, 0), (3, 0)]
    near = [(0, dt) for dt in chips[1:]]
    far = [(dz, dt) for dz in (2, 3) for dt in chips[1:]]
    side = [(1, dt) for dt in chips]
    order = lead + near + far + side
    batches = [
        [(0, 0)] + near,
        lead,
        [(2, 2), (2, 4)],
        [(2, 6), (3, 2)],
        [(1, 0), (1, 2)],
        [(3, 4), (1, 4)],
    ]
    last = [(3, 6), (1, 6)]
    got = {}
    sent = dict(zip(lead, pick(lead, bricks, weights, aperture, owners)))
    rest = [(0, 0)] + order[len(lead) :]
    sent.update(zip(rest, pick(rest, bricks, weights, aperture, owners)))
    got[0, 0] = sent[0, 0]
    for key in order:
        got[key] = permute(sent[key], *key)
    images = []
    for batch in batches:
        messages = [got[key] for key in batch]
        images = image_step(messages, None, images, columns, group)
    mine, other = images
    late = [got[key] for key in last]
    other = permute(other, 0, 1)
    relayed = permute(jnp.concatenate([m[SIDE:] for m in late], axis=0), 0, 1)
    (mine,) = image_step(late, None, [mine], columns, group, sides=1)
    image, _ = image_step([], relayed, [mine, other], columns, group, final=True, sides=1)
    return image.reshape(group, 2 * SUB, FINE, 2 * BZ)


def solution(mesh):
    placed = (
        P(("src", "tile"), None, None, None),
        P(("src", "tile"), None),
        P(("src", "tile"), None),
    )
    quarters, owners = mesh.shape["src"], mesh.shape["tile"]
    fits = quarters == 4 and BX == quarters * SUB and owners == 8
    return jax.shard_map(
        octet_shards if fits else general_shards,
        mesh=mesh,
        in_specs=placed,
        out_specs=P("tile", "src", None, None),
        check_vma=False,
    )
```

```python
import functools
import math

import jax
import jax.numpy as jnp
import numpy as np
from jax import lax
from jax.experimental import pallas as pl
from jax.experimental.pallas import tpu as pltpu
from jax.sharding import PartitionSpec as P


BX = 32
BY = 16
BZ = 64
SUB = 8
LANES = 128

angular_rate = 9.0


def refine_axis(values, axis):
    length = values.shape[axis]
    first = lax.slice_in_dim(values, 0, 1, axis=axis)
    last = lax.slice_in_dim(values, length - 1, length, axis=axis)
    lower = jnp.concatenate([first, lax.slice_in_dim(values, 0, length - 1, axis=axis)], axis=axis)
    upper = jnp.concatenate([lax.slice_in_dim(values, 1, length, axis=axis), last], axis=axis)
    even_rows = 0.75 * values + 0.25 * lower
    odd_rows = 0.75 * values + 0.25 * upper
    paired = jnp.stack([even_rows, odd_rows], axis=axis + 1)
    shape = values.shape[:axis] + (2 * length,) + values.shape[axis + 1 :]
    return paired.reshape(shape)


def refine_accumulate(coarse, details, fine_rows, tile_count):
    items = coarse.shape[0]
    turns = 8
    block = items // turns
    coarse_rows = coarse.shape[1]
    tile_ids = jnp.arange(tile_count).astype(jnp.float32)

    def one_block(total, item):
        bricks, info = item
        shaped = bricks.reshape(block, coarse_rows, BY, BZ)
        along_x = refine_axis(shaped, 1)
        along_z = refine_axis(along_x, 3)
        fine = refine_axis(along_z, 2)
        phase = jnp.cos(angular_rate * fine)
        select = (info[:, 1:2] == tile_ids[None, :]).astype(jnp.float32) * info[:, 0:1]
        total = total + jnp.einsum("kp,kfyz->pfyz", select, phase, precision=lax.Precision.HIGHEST)
        return (total, None)

    stacked = (
        coarse.reshape(turns, block, coarse_rows, coarse.shape[2]),
        details.reshape(turns, block, 2),
    )
    start = jnp.zeros((tile_count, fine_rows, 2 * BY, 2 * BZ), jnp.float32)
    total, _ = lax.scan(one_block, start, stacked)
    return total


def general_shards(tables, weights, aperture):
    bricks = tables[0]
    own_weight = weights[0]
    own_mask = aperture[0]
    owners = lax.axis_size("tile")
    group = bricks.shape[0] // owners
    capacity = group // 2
    plane = bricks.shape[2]
    live = own_mask.reshape(owners, group)
    ranking = jnp.cumsum(live, axis=1) - 1
    slot_ids = jnp.arange(capacity)
    chosen = ((live[:, None, :] == 1) & (ranking[:, None, :] == slot_ids[None, :, None])).astype(
        jnp.int32
    )
    local_tile = jnp.sum(chosen * jnp.arange(group)[None, None, :], axis=2)
    occupied = jnp.sum(chosen, axis=2)
    brick_index = local_tile + jnp.arange(owners)[:, None] * group
    picked = bricks[brick_index]
    factor = own_weight[brick_index] * occupied.astype(jnp.float32)
    details = jnp.stack([factor, local_tile.astype(jnp.float32)], axis=-1)
    arrived, info = (
        lax.all_to_all(picked, "tile", split_axis=0, concat_axis=0, tiled=True),
        lax.all_to_all(details, "tile", split_axis=0, concat_axis=0, tiled=True),
    )
    partial_image = refine_accumulate(
        arrived.reshape(-1, BX, plane), info.reshape(-1, 2), 2 * BX, group
    )
    return lax.psum_scatter(partial_image, "src", scatter_dimension=1, tiled=True)


YP = BY * BZ // LANES
BLOCK = YP + 2
SLOTS = 2
SIDE = SLOTS * BLOCK
MESSAGE = 2 * SIDE + 1
FINE = 2 * BY


def cos_series():
    nodes = 400
    v = 0.125 + 0.125 * np.cos(np.pi * (np.arange(nodes) + 0.5) / nodes)
    cheb = np.polynomial.chebyshev.Chebyshev.fit(
        v, np.cos(2 * np.pi * np.sqrt(v)), 5, domain=[0.0, 0.25]
    )
    return [float(c) for c in cheb.convert(kind=np.polynomial.Polynomial, domain=[-1, 1]).coef]


def refine_columns():
    m = np.zeros((2 * BZ, BZ), np.float64)
    for i in range(2 * BZ):
        k = i // 2
        other = max(k - 1, 0) if i % 2 == 0 else min(k + 1, BZ - 1)
        m[i, k] += 0.75
        m[i, other] += 0.25
    out = np.zeros((2, 2, BZ, 2, 2, 2 * BZ), np.float64)
    for split in range(2):
        for scale, factor in enumerate((0.75, 0.25)):
            for parity in range(2):
                out[split, parity, :, scale, parity, :] = factor * m.T
    return out.reshape(4 * BZ, 8 * BZ)


def slot_scalars(mask_ref, weight_ref, first, group, slot):
    count = jnp.int32(0)
    local = jnp.int32(0)
    weight = jnp.float32(0.0)
    for i in range(group):
        live = mask_ref[0, first + i] == 1
        hit = jnp.logical_and(live, count == slot)
        local = jnp.where(hit, jnp.int32(i), local)
        weight = jnp.where(hit, weight_ref[0, first + i], weight)
        count = count + live.astype(jnp.int32)
    return local, weight


def pick_kernel(sends, quarters, group, mask_in, weight_in, tables_ref, *refs):
    outs, (mask_ref, weight_ref, small, buf, sem) = refs[: len(sends)], refs[len(sends) :]
    heads = [
        pltpu.make_async_copy(mask_in, mask_ref, small.at[0]),
        pltpu.make_async_copy(weight_in, weight_ref, small.at[1]),
    ]
    for head in heads:
        head.start()
    r, t = lax.axis_index("src"), lax.axis_index("tile")
    offsets = sorted({dt ^ side for _, dt in sends for side in range(2)})
    ahead = buf.shape[0] == len(offsets) * group
    copies = []
    if ahead:
        for n, offset in enumerate(offsets):
            for i in range(group):
                s = n * group + i
                copy = pltpu.make_async_copy(
                    tables_ref.at[(t ^ offset) * group + i], buf.at[s], sem.at[s]
                )
                copy.start()
                copies.append(copy)
    for head in heads:
        head.wait()
    lanes = lax.broadcasted_iota(jnp.int32, (SUB, LANES), 1)
    found = {}
    for n, offset in enumerate(offsets):
        g = t ^ offset
        for j in range(SLOTS):
            local, weight = slot_scalars(mask_ref, weight_ref, g * group, group, j)
            if ahead:
                found[offset, j] = (n * group + local, local, weight)
                continue
            s = n * SLOTS + j
            found[offset, j] = (s, local, weight)
            copy = pltpu.make_async_copy(tables_ref.at[g * group + local], buf.at[s], sem.at[s])
            copy.start()
            copies.append(copy)
    for out_ref, (dz, dt) in zip(outs, sends):
        info = jnp.zeros((SUB, LANES), jnp.float32)
        for side in range(1 if out_ref.shape[0] <= SIDE + 1 else 2):
            for j in range(SLOTS):
                _, local, weight = found[dt ^ side, j]
                lane = 2 * (side * SLOTS + j)
                info = jnp.where(lanes == lane, weight, info)
                info = jnp.where(lanes == lane + 1, local.astype(jnp.float32), info)
        out_ref[SIDE] = info
    for copy in copies:
        copy.wait()
    for out_ref, (dz, dt) in zip(outs, sends):
        q = r ^ dz
        below, above = jnp.maximum(q - 1, 0), jnp.minimum(q + 1, quarters - 1)
        for side in range(1 if out_ref.shape[0] <= SIDE + 1 else 2):
            for j in range(SLOTS):
                s = found[dt ^ side, j][0]
                first = side * (SIDE + 1) + j * BLOCK
                for y in range(YP):
                    at = slice(y * LANES, (y + 1) * LANES)
                    out_ref[first + y] = buf[s, q, :, at]
                    out_ref[first + YP, y : y + 1, :] = jnp.where(
                        q > 0, buf[s, below, SUB - 1 : SUB, at], buf[s, below, 0:1, at]
                    )
                    out_ref[first + YP + 1, y : y + 1, :] = jnp.where(
                        q < quarters - 1, buf[s, above, 0:1, at], buf[s, above, SUB - 1 : SUB, at]
                    )


def pick(sends, single, bricks, weights, aperture, owners):
    group = bricks.shape[0] // owners
    quarters = bricks.shape[1]
    needed = len({dt ^ side for _, dt in sends for side in range(2)})
    slots = needed * (group if needed == 2 else SLOTS)
    home = functools.partial(pltpu.with_memory_space_constraint, memory_space=pltpu.HBM)
    return pl.pallas_call(
        functools.partial(pick_kernel, sends, quarters, group),
        out_shape=[
            pltpu.VMEM((SIDE + 1 if key in single else MESSAGE, SUB, LANES), jnp.float32)
            for key in sends
        ],
        in_specs=[pl.BlockSpec(memory_space=pltpu.HBM)] * 3,
        out_specs=[pl.BlockSpec(memory_space=pltpu.VMEM) for _ in sends],
        scratch_shapes=[
            pltpu.SMEM(aperture.shape, aperture.dtype),
            pltpu.SMEM(weights.shape, weights.dtype),
            pltpu.SemaphoreType.DMA((2,)),
            pltpu.VMEM((slots,) + bricks.shape[1:], jnp.float32),
            pltpu.SemaphoreType.DMA((slots,)),
        ],
        compiler_params=pltpu.CompilerParams(vmem_limit_bytes=16 << 20),
    )(home(aperture), home(weights), home(bricks))


def refine_side(ref, base, columns_ref, res_ref):
    rows = lax.broadcasted_iota(jnp.int32, (SUB, LANES), 0)
    turns = angular_rate / (2 * math.pi)
    near, away = 0.75 * turns, 0.25 * turns
    parts = []
    for j in range(SLOTS):
        even, odd = [], []
        for y in range(YP):
            first = base + j * BLOCK
            c = ref[first + y]
            low = jnp.broadcast_to(ref[first + YP, y : y + 1, :], c.shape)
            high = jnp.broadcast_to(ref[first + YP + 1, y : y + 1, :], c.shape)
            mid = near * c
            even.append(mid + away * jnp.where(rows == 0, low, pltpu.roll(c, 1, 0)))
            odd.append(mid + away * jnp.where(rows == SUB - 1, high, pltpu.roll(c, SUB - 1, 0)))
        parts += even + odd
    x = jnp.concatenate(parts, axis=0)
    top = x.astype(jnp.bfloat16)
    rest = (x - top.astype(jnp.float32)).astype(jnp.bfloat16)
    res_ref[...] = jnp.dot(
        jnp.concatenate([top, rest], axis=1), columns_ref[...], preferred_element_type=jnp.float32
    )


def add_slot(acc_ref, series, res_ref, j, weight, tile):
    scaled = [weight * c for c in series]
    for parity in range(2):

        def part(pair, k):
            r = ((j * 2 + parity) * YP + pair) * SUB
            return res_ref[r : r + SUB, k * LANES : (k + 1) * LANES]

        for y in range(FINE):
            pair, k = divmod(y, 4)
            if k == 0:
                t = part(pair, 0) + (part(pair - 1, 3) if pair > 0 else part(pair, 2))
            elif k == 1:
                t = part(pair, 0) + part(pair, 3)
            elif k == 2:
                t = part(pair, 1) + part(pair, 2)
            else:
                t = part(pair, 1) + (part(pair + 1, 2) if pair < YP - 1 else part(pair, 3))
            r = t - jnp.round(t)
            u = r * r
            p = scaled[5]
            for c in scaled[4::-1]:
                p = p * u + c
            at = slice((parity * FINE + y) * SUB, (parity * FINE + y + 1) * SUB)
            acc_ref[tile, at, :] = acc_ref[tile, at, :] + p


def image_kernel(entries, rows, arrays, sides, first, final, group, *refs):
    ins, columns_ref, refs = refs[:arrays], refs[arrays], refs[arrays + 1 :]
    if final:
        other_ref, refs = refs[1], refs[2:]
        out_ref, acc, refs = refs[0], refs[1:2], refs[2:]
        stage, out_sem, refs = refs[0], refs[1], refs[2:]
    else:
        refs = refs if first else refs[sides:]
        acc, refs = refs[:sides], refs[sides:]
    info, sem, res = refs[0], refs[1], refs[2:]
    copies = [
        pltpu.make_async_copy(ins[which].at[tile, pl.ds(0, 1), :], info.at[k], sem.at[k])
        for k, (which, tile) in enumerate(rows)
    ]
    for copy in copies:
        copy.start()
    series = cos_series()
    refine_side(ins[entries[0][0]], entries[0][1], columns_ref, res[0])
    if first:
        for image in acc:

            def clear(k, carry):
                image[k] = jnp.zeros(image.shape[1:], jnp.float32)
                return carry

            lax.fori_loop(0, group, clear, 0)
    for copy in copies:
        copy.wait()
    for n, entry in enumerate(entries):
        if n + 1 < len(entries):
            later = entries[n + 1]
            refine_side(ins[later[0]], later[1], columns_ref, res[(n + 1) % 2])
        for j in range(SLOTS):
            weight = info[entry[2], 0, entry[3] + 2 * j]
            tile = info[entry[2], 0, entry[3] + 2 * j + 1].astype(jnp.int32)
            add_slot(acc[entry[4]], series, res[n % 2], j, weight, tile)

    if final:
        written = []
        for k in range(group):
            for parity in range(2):
                for x in range(SUB):
                    for y in range(0, FINE, SUB):
                        at = pl.ds((parity * FINE + y) * SUB + x, SUB, stride=SUB)
                        row = (2 * x + parity) * FINE + y
                        stage[k, row : row + SUB, :] = acc[0][k, at, :] + other_ref[k, at, :]
            copy = pltpu.make_async_copy(stage.at[k], out_ref.at[k], out_sem.at[k])
            copy.start()
            written.append(copy)
        for copy in written:
            copy.wait()


def image_step(messages, relayed, images, columns, group, final=False, sides=2):
    near = functools.partial(pltpu.with_memory_space_constraint, memory_space=pltpu.VMEM)
    entries, arrays, rows = [], [], []
    for m in messages:
        for side in range(sides):
            entries.append((len(arrays), side * (SIDE + 1), len(rows), side * 2 * SLOTS, side))
        rows.append((len(arrays), SIDE))
        arrays.append(m)
    if relayed is not None:
        for first in range(0, relayed.shape[0], SIDE + 1):
            entries.append((len(arrays), first + 1, len(rows), 2 * SLOTS, 0))
            rows.append((len(arrays), first))
        arrays.append(relayed)
    shape = (group, 2 * FINE * SUB, LANES)
    whole = pl.BlockSpec(memory_space=pltpu.VMEM)
    scratch = [
        pltpu.SMEM((len(rows), 1, LANES), jnp.float32),
        pltpu.SemaphoreType.DMA((len(rows),)),
        pltpu.VMEM((SLOTS * 2 * YP * SUB, 4 * LANES), jnp.float32),
        pltpu.VMEM((SLOTS * 2 * YP * SUB, 4 * LANES), jnp.float32),
    ]
    kept = len(arrays) + 1
    if final:
        out_shape = [jax.ShapeDtypeStruct(shape, jnp.float32), pltpu.VMEM(shape, jnp.float32)]
        out_specs = [pl.BlockSpec(memory_space=pltpu.HBM), whole]
        scratch = [pltpu.VMEM(shape, jnp.float32), pltpu.SemaphoreType.DMA((group,))] + scratch
        aliases = {kept: 1}
    else:
        out_shape = [pltpu.VMEM(shape, jnp.float32)] * sides
        out_specs = [whole] * sides
        aliases = {kept + k: k for k in range(len(images))}
    return pl.pallas_call(
        functools.partial(
            image_kernel, entries, rows, len(arrays), sides, not images, final, group
        ),
        out_shape=out_shape,
        in_specs=[whole] * (kept + len(images)),
        out_specs=out_specs,
        scratch_shapes=scratch,
        input_output_aliases=aliases,
        compiler_params=pltpu.CompilerParams(vmem_limit_bytes=16 << 20),
    )(*[near(a) for a in arrays], near(columns), *[near(a) for a in images])


def octet_shards(tables, weights, aperture):
    quarters, owners = lax.axis_size("src"), lax.axis_size("tile")
    group = tables.shape[1] // owners
    columns = jnp.asarray(refine_columns(), jnp.bfloat16)
    bricks = tables[0].reshape(-1, quarters, SUB, YP * LANES)

    def permute(value, dz, dt):
        def other(r, t):
            return (r ^ dz) * owners + (t ^ dt)

        pairs = [(r * owners + t, other(r, t)) for r in range(quarters) for t in range(owners)]
        return lax.ppermute(value, ("src", "tile"), pairs)

    chips = range(0, owners, 2)
    lead = [(2, 0), (3, 0)]
    near = [(0, dt) for dt in chips[1:]]
    late = [(3, 4), (3, 5), (1, 6), (1, 7)]
    last = [[(3, 6), (3, 7)], [(1, 4), (1, 5)]]
    single = set(late + last[0] + last[1])
    far = [(2, 2), (2, 4), (2, 6), (3, 2)] + late[:2] + last[0]
    side = [(1, 0), (1, 2)] + late[2:] + last[1]
    order = lead + near + far + side
    batches = [[(0, 0)] + near, lead, [(2, 2), (2, 4)], [(2, 6), (3, 2)], [(1, 0), (1, 2)]]
    got = {}
    sent = dict(zip(lead, pick(lead, single, bricks, weights, aperture, owners)))
    rest = [(0, 0)] + order[len(lead) :]
    sent.update(zip(rest, pick(rest, single, bricks, weights, aperture, owners)))
    got[0, 0] = sent[0, 0]
    for key in order:
        got[key] = permute(sent[key], *key)
    images = []
    for batch in batches:
        messages = [got[key] for key in batch]
        images = image_step(messages, None, images, columns, group)
    mine, other = images
    other = permute(other, 0, 1)
    for batch in (late, last[0]):
        messages = [got[key] for key in batch]
        (mine,) = image_step(messages, None, [mine], columns, group, sides=1)
    image, _ = image_step(
        [got[key] for key in last[1]], None, [mine, other], columns, group,
        final=True, sides=1,
    )
    return image.reshape(group, 2 * SUB, FINE, 2 * BZ)


def solution(mesh):
    placed = (
        P(("src", "tile"), None, None, None),
        P(("src", "tile"), None),
        P(("src", "tile"), None),
    )
    quarters, owners = mesh.shape["src"], mesh.shape["tile"]
    fits = quarters == 4 and BX == quarters * SUB and owners == 8
    return jax.shard_map(
        octet_shards if fits else general_shards,
        mesh=mesh,
        in_specs=placed,
        out_specs=P("tile", "src", None, None),
        check_vma=False,
    )
```
